32 devices in a mesh: group: 8 (over y, x, core), head: 4 (over z).
Axes of the slice: x: 2, y: 2, z: 4, core: 2. Of those that a mesh axis runs over, the one named last changes fastest.
Arguments:
- hidden_in: bfloat16 [128, 2560], P('group'), may hold values from -6 to 6
- ssm_state: float32 [128, 80, 64, 128], P('group', 'head'), may hold values from -6 to 6
- conv_x_state: bfloat16 [128, 3, 5120], P('group', None, 'head'), may hold values from -6 to 6
- conv_bc_state: bfloat16 [128, 3, 256], P('group'), may hold values from -6 to 6
- token_ids: int32 [128], P('group'), may hold values from 0 to 25599
- ref_logits: bfloat16 [128, 25600], P('group', 'head'), may hold values from -15 to 350
- in_z: bfloat16 [2560, 5120], P('group', 'head'), may hold values from -0.125 to 0.125
- in_x: bfloat16 [2560, 5120], P('group', 'head'), may hold values from -0.125 to 0.125
- in_bc: bfloat16 [2560, 256], P('group'), may hold values from -0.125 to 0.125
- in_dt: bfloat16 [2560, 80], P('group', 'head'), may hold values from -0.125 to 0.125
- out_t: bfloat16 [2560, 5120], P('group', 'head'), may hold values from -0.078125 to 0.078125
- lm_head: bfloat16 [25600, 2560], P('head', 'group'), may hold values from -6 to 6
- conv_wx: float32 [4, 5120], P(None, 'head'), may hold values from -3 to 3
- conv_bx: float32 [5120], P('head'), may hold values from -1.5 to 1.5
- conv_wbc: float32 [4, 256], replicated, may hold values from -3 to 3
- conv_bbc: float32 [256], replicated, may hold values from -1.5 to 1.5
- dt_bias: float32 [80], P('head'), may hold values from -4 to -1
- a_log: float32 [80], P('head'), may hold values from 0 to 2.77
- skip_gain: float32 [80], P('head'), may hold values from 0.5 to 1.5
- norm_in: float32 [2560], replicated, may hold values from 0.5 to 1.5
- norm_gain: float32 [5120], P('head'), may hold values from 0.5 to 1.5
- final_gain: float32 [2560], replicated, may hold values from 0.5 to 1.5
Outputs:
- new_state: float32 [128, 80, 64, 128], P('group', 'head')
- divergence: float32 [128], P('group')
- token_logprob: float32 [128], P('group')
- roll_z: bfloat16 [2560, 5120], P(None, 'head')
- roll_x: bfloat16 [2560, 5120], P(None, 'head')
- roll_bc: bfloat16 [2560, 256], replicated
- roll_dt: bfloat16 [2560, 80], P(None, 'head')
- roll_out: bfloat16 [2560, 5120], P(None, 'head')
The draws below stay inside these ranges and needn't reach their ends.
All inputs are finite; a program needn't handle non-finite values.
Results may differ from the reference program's by a relative error of at most 0.0102.
Values may be sent and summed in bfloat16 or wider, within the bound.
A program may use at most 128 MiB of HBM per device.

```python
import math
import jax
import jax.numpy as jnp
from jax import lax

D = 2560
H = 80
P_SIZE = 64
N = 128
KCONV = 4
V = 25600
SEQS = 16
DI = 5120
SEQ_ALL = 128
N_GROUP = 8


def draw_lm_head(key, part):
    subkeys = jax.random.split(key, 1)
    values = jax.random.normal(subkeys[0], (V, D), jnp.float32) * (3.0 / math.sqrt(D))
    return jnp.clip(values, -6.0, 6.0).astype(jnp.bfloat16)


def draw_ref_logits(key, part):
    subkeys = jax.random.split(key, 1)
    total_rows = SEQS * N_GROUP
    values = jnp.clip(jax.random.normal(subkeys[0], (total_rows, V), jnp.float32) * 3.0, -15.0, 15.0)
    return values.astype(jnp.bfloat16)


def place_ends(drawn, key, least, largest):
    place = [jax.random.randint(jax.random.fold_in(key, axis), (), 0, length) for axis, length in enumerate(drawn.shape)]
    longest = drawn.shape.index(max(drawn.shape))
    neighbour = place[:longest] + [(place[longest] + 1) % drawn.shape[longest]] + place[longest + 1:]
    return drawn.at[tuple(place)].set(least).at[tuple(neighbour)].set(largest)


def level_of(key, shape, pieces, smallest, top_value):
    level = 1.0
    for axis_at, shards_of in pieces:
        steps = jax.random.uniform(jax.random.fold_in(jax.random.fold_in(key, 6), axis_at), (shards_of,), jnp.float32, smallest / len(pieces), top_value / len(pieces))
        level = level * jnp.repeat(jnp.exp(steps), shape[axis_at] // shards_of).reshape((-1,) + (1,) * (len(shape) - 1 - axis_at))
    return level


def scatter_about(key, extent, scale, limit, pieces=(), held_as=jnp.bfloat16):
    entries = scale * jax.random.normal(key, extent, jnp.float32)
    if pieces:
        entries = entries * level_of(key, extent, pieces, -0.22, 0.18)
    return jnp.clip(entries, -limit, limit).astype(held_as)


def setup_inputs(seed: int = 0) -> dict:
    arg_keys = jax.random.split(jax.random.key(seed), 23)
    hidden_in = scatter_about(arg_keys[0], (SEQ_ALL, D), 1.0, 6.0, ((0, 8),))
    ssm_state = scatter_about(arg_keys[1], (SEQ_ALL, H, P_SIZE, N), 1.0, 6.0, ((0, 8), (1, 4)), jnp.float32)
    conv_x_state = scatter_about(arg_keys[2], (SEQ_ALL, KCONV - 1, DI), 1.0, 6.0, ((0, 8), (2, 4)))
    conv_bc_state = scatter_about(arg_keys[3], (SEQ_ALL, KCONV - 1, 2 * N), 1.0, 6.0, ((0, 8),))
    token_ids = place_ends(jax.random.randint(arg_keys[4], (SEQ_ALL,), 0, V), jax.random.fold_in(arg_keys[4], 1), 0, V - 1).astype(jnp.int32)
    ref_logits = draw_ref_logits(jax.random.fold_in(arg_keys[22], 71), 0)
    in_z = scatter_about(arg_keys[6], (D, DI), D ** -0.5, 0.125, ((0, 8), (1, 4)))
    in_x = scatter_about(arg_keys[7], (D, DI), D ** -0.5, 0.125, ((0, 8), (1, 4)))
    in_bc = scatter_about(arg_keys[8], (D, 2 * N), D ** -0.5, 0.125, ((0, 8),))
    in_dt = scatter_about(arg_keys[9], (D, H), D ** -0.5, 0.125, ((0, 8), (1, 4)))
    out_t = scatter_about(arg_keys[10], (D, DI), DI ** -0.5, 0.078125, ((0, 8), (1, 4)))
    lm_head = draw_lm_head(jax.random.fold_in(arg_keys[22], 71), 0)
    conv_wx = scatter_about(arg_keys[12], (KCONV, DI), KCONV ** -0.5, 3.0, ((1, 4),), jnp.float32)
    conv_bx = scatter_about(arg_keys[13], (DI,), 0.3, 1.5, ((0, 4),), jnp.float32)
    conv_wbc = scatter_about(arg_keys[14], (KCONV, 2 * N), KCONV ** -0.5, 3.0, (), jnp.float32)
    conv_bbc = scatter_about(arg_keys[15], (2 * N,), 0.3, 1.5, (), jnp.float32)
    dt_bias = jnp.clip(-4.0 + 3.0 * jax.random.uniform(arg_keys[16], (H,), jnp.float32) ** level_of(arg_keys[16], (H,), ((0, 4),), -0.2, 0.2), -4.0, -1.0)
    a_log = jnp.clip(2.77 * jax.random.uniform(arg_keys[17], (H,), jnp.float32) ** level_of(arg_keys[17], (H,), ((0, 4),), -0.2, 0.2), 0.0, 2.77)
    skip_gain = jnp.clip(0.5 + 1.0 * jax.random.uniform(arg_keys[18], (H,), jnp.float32) ** level_of(arg_keys[18], (H,), ((0, 4),), -0.2, 0.2), 0.5, 1.5)
    norm_in = jnp.clip(1.0 + 0.1 * jax.random.normal(arg_keys[19], (D,), jnp.float32), 0.5, 1.5)
    norm_gain = jnp.clip(1.0 + 0.1 * jax.random.normal(arg_keys[20], (DI,), jnp.float32), 0.5, 1.5)
    final_gain = jnp.clip(1.0 + 0.1 * jax.random.normal(arg_keys[21], (D,), jnp.float32), 0.5, 1.5)
    return {"hidden_in": hidden_in, "ssm_state": ssm_state, "conv_x_state": conv_x_state, "conv_bc_state": conv_bc_state, "token_ids": token_ids, "ref_logits": ref_logits, "in_z": in_z, "in_x": in_x, "in_bc": in_bc, "in_dt": in_dt, "out_t": out_t, "lm_head": lm_head, "conv_wx": conv_wx, "conv_bx": conv_bx, "conv_wbc": conv_wbc, "conv_bbc": conv_bbc, "dt_bias": dt_bias, "a_log": a_log, "skip_gain": skip_gain, "norm_in": norm_in, "norm_gain": norm_gain, "final_gain": final_gain}


EPSILON = 1e-05

def rms_norm(values, gain):
    return values * lax.rsqrt(lax.optimization_barrier(jnp.mean(values * values, axis=-1, keepdims=True)) + EPSILON) * gain

def causal_conv(history, newest, taps, offset):
    window = jnp.concatenate([history, newest[:, None, :]], axis=1).astype(jnp.float32)
    return jax.nn.silu(lax.optimization_barrier(jnp.sum(window * taps[None, :, :], axis=1)) + offset)

def reference(hidden_in, ssm_state, conv_x_state, conv_bc_state, token_ids, ref_logits, in_z, in_x, in_bc, in_dt, out_t, lm_head, conv_wx, conv_bx, conv_wbc, conv_bbc, dt_bias, a_log, skip_gain, norm_in, norm_gain, final_gain):
    stream_in = hidden_in.astype(jnp.float32)
    normed = rms_norm(stream_in, norm_in).astype(jnp.bfloat16)
    gate_branch = jnp.dot(normed, in_z, preferred_element_type=jnp.float32).astype(jnp.bfloat16)
    x_branch = jnp.dot(normed, in_x, preferred_element_type=jnp.float32).astype(jnp.bfloat16)
    bc_branch = jnp.dot(normed, in_bc, preferred_element_type=jnp.float32).astype(jnp.bfloat16)
    step_raw = jnp.dot(normed, in_dt, preferred_element_type=jnp.float32).astype(jnp.bfloat16)
    x_conv = causal_conv(conv_x_state, x_branch, conv_wx, conv_bx)
    bc_conv = causal_conv(conv_bc_state, bc_branch, conv_wbc, conv_bbc)
    b_vals = bc_conv[:, :N]
    c_vals = bc_conv[:, N:]
    step = jax.nn.softplus(step_raw.astype(jnp.float32) + dt_bias)
    decay = jnp.exp(-step * jnp.exp(a_log))
    seq_count = x_conv.shape[0]
    x_heads = x_conv.reshape(seq_count, H, P_SIZE)
    inflow = (step[:, :, None] * x_heads)[:, :, :, None] * b_vals[:, None, None, :]
    new_state = decay[:, :, None, None] * ssm_state + inflow
    ssm_out = jnp.einsum('shpn,sn->shp', new_state, c_vals, precision=lax.Precision.HIGHEST)
    ssm_out = (ssm_out + skip_gain[None, :, None] * x_heads).reshape(seq_count, H * P_SIZE)
    gated = ssm_out * jax.nn.silu(gate_branch.astype(jnp.float32))
    gated_out = rms_norm(gated, norm_gain).astype(jnp.bfloat16)
    mixed = lax.dot_general(gated_out, out_t, (((1,), (1,)), ((), ())), preferred_element_type=jnp.float32)
    final_hidden = rms_norm(stream_in + mixed, final_gain).astype(jnp.bfloat16)
    logits = lax.dot_general(final_hidden, lm_head, (((1,), (1,)), ((), ())), preferred_element_type=jnp.float32)
    lse_roll = jax.nn.logsumexp(logits, axis=-1)
    reference_rows = ref_logits.astype(jnp.float32)
    lse_ref = jax.nn.logsumexp(reference_rows, axis=-1)
    log_ref = reference_rows - lse_ref[:, None]
    divergence = lax.optimization_barrier(jnp.sum(jnp.exp(log_ref) * (log_ref - (logits - lse_roll[:, None])), axis=-1))
    picked = jnp.take_along_axis(logits, token_ids[:, None].astype(jnp.int32), axis=1)[:, 0]
    token_logprob = picked - lse_roll
    return (new_state, divergence, token_logprob, in_z, in_x, in_bc, in_dt, out_t)
```

```python
import functools

import jax
import jax.numpy as jnp
from jax import lax
from jax.experimental import pallas as pl
from jax.experimental.pallas import tpu as pltpu
from jax.sharding import PartitionSpec as P

P_SIZE = 64
EPSILON = 1e-05
MESH = pl.DeviceIdType.MESH


def rms_norm(values, gain):
    return values * lax.rsqrt(jnp.mean(values * values, axis=-1, keepdims=True) + EPSILON) * gain


def causal_conv(history, newest, taps, offset):
    window = jnp.concatenate([history, newest[:, None, :]], axis=1).astype(jnp.float32)
    return jax.nn.silu(jnp.sum(window * taps[None, :, :], axis=1) + offset)


def flip(value, mask):
    bit = 1
    while bit <= mask:
        if mask & bit:
            value = value + bit * (1 - 2 * ((value // bit) % 2))
        bit *= 2
    return value


class Gather:
    def __init__(self, chips, ins, outs, local, send, recv, psend, precv):
        self.chips, self.ins, self.outs = chips, ins, outs
        self.local, self.send, self.recv, self.psend, self.precv = local, send, recv, psend, precv
        group = lax.axis_index("group")
        self.chip, self.core = group // 2, group % 2
        self.pending = []
        self.relay = chips == 4

    def rows(self, a, chip, core, part=None):
        count = self.ins[a].shape[0]
        start = (chip * 2 + core) * count
        if part is not None:
            count = count // 2
            start = start + part * count
        return pl.ds(pl.multiple_of(start, 16), count)

    def copy(self, src, dst, chip, core, ssem, rsem):
        made = pltpu.make_async_remote_copy(
            src_ref=src, dst_ref=dst, send_sem=ssem, recv_sem=rsem,
            device_id={"group": chip * 2 + core}, device_id_type=MESH,
        )
        made.start()
        self.pending.append(made)
        return made

    def start(self, a):
        src = self.ins[a]
        own = self.outs[a].at[self.rows(a, self.chip, self.core)]
        loc = pltpu.make_async_copy(src, own, self.local.at[a])
        loc.start()
        self.far = getattr(self, "far", {})
        peers = [1, 2] if self.relay else range(1, self.chips)
        for m in peers:
            self.far[a, m] = self.copy(
                src, own, flip(self.chip, m), self.core, self.send.at[a, m], self.recv.at[a, m])
        self.near = getattr(self, "near", {})
        self.near[a, 0] = self.copy(
            src, own, self.chip, 1 - self.core, self.psend.at[a, 0], self.precv.at[a, 0])
        self.locals = getattr(self, "locals", {})
        self.locals[a] = loc

    def hand_on(self, a, m, chip, part, slot):
        view = self.outs[a].at[self.rows(a, chip, self.core, part)]
        self.near[a, slot] = self.copy(
            view, view, self.chip, 1 - self.core, self.psend.at[a, slot], self.precv.at[a, slot])

    def relay_near(self, a):
        if self.relay:
            for m, part in ((1, 0), (2, 1)):
                self.far[a, m].wait_recv()
                source = flip(self.chip, m)
                view = self.outs[a].at[self.rows(a, source, self.core, part)]
                self.far[a, 3 + part] = self.copy(
                    view, view, flip(self.chip, 3 - m), self.core,
                    self.send.at[a, 3 + part], self.recv.at[a, 3 + part])
                self.hand_on(a, m, source, None, m)
        else:
            for m in range(1, self.chips):
                self.far[a, m].wait_recv()
                self.hand_on(a, m, flip(self.chip, m), None, m)

    def relay_far(self, a):
        if self.relay:
            for part in (0, 1):
                self.far[a, 3 + part].wait_recv()
                self.hand_on(a, 3, flip(self.chip, 3), part, 3 + part)

    def arrive(self, a):
        for (b, _), made in self.near.items():
            if b == a:
                made.wait_recv()
        self.locals[a].wait()

    def drain(self):
        for made in self.pending:
            made.wait_send()


def gather_sems(count, chips):
    slots = max(chips, 5)
    dma = pltpu.SemaphoreType.DMA
    return [dma((count,)), dma((count, slots)), dma((count, slots)), dma((count, slots)), dma((count, slots))]


def greet(groups, heads):
    barrier = pltpu.get_barrier_semaphore()
    group, head = lax.axis_index("group"), lax.axis_index("head")
    for j in range(1, groups):
        pl.semaphore_signal(barrier, inc=1, device_id={"group": (group + j) % groups}, device_id_type=MESH)
    for j in range(1, heads):
        pl.semaphore_signal(barrier, inc=1, device_id={"head": (head + j) % heads}, device_id_type=MESH)
    pl.semaphore_wait(barrier, groups - 1 + heads - 1)


def gather_kernel(groups, count, *refs):
    ins, outs, sems = refs[:count], refs[count:2 * count], refs[2 * count:]
    work = Gather(groups // 2, ins, outs, *sems)
    greet(groups, 1)
    for a in range(count):
        work.start(a)
    for a in range(count):
        work.relay_near(a)
        if a:
            work.relay_far(a - 1)
    work.relay_far(count - 1)
    for a in range(count):
        work.arrive(a)
    work.drain()


def gather(groups, arrays):
    count = len(arrays)
    any_spec = pl.BlockSpec(memory_space=pl.ANY)
    return pl.pallas_call(
        functools.partial(gather_kernel, groups, count),
        out_shape=[jax.ShapeDtypeStruct((groups * v.shape[0], v.shape[1]), v.dtype) for v in arrays],
        in_specs=[any_spec] * count,
        out_specs=[any_spec] * count,
        scratch_shapes=gather_sems(count, groups // 2),
        compiler_params=pltpu.CompilerParams(collective_id=0, has_side_effects=True),
        name="gather_in",
    )(*arrays)


def state_kernel(decay_ref, inflow_ref, b_ref, c_ref, state_ref, new_ref, y_ref):
    def column(row, other):
        first = lax.broadcasted_iota(jnp.int32, (8, row.shape[1]), 0) == 0
        left = jnp.where(first, jnp.broadcast_to(row, (8, row.shape[1])), 0.0)
        right = jnp.broadcast_to(other, (8, other.shape[1]))
        return lax.dot_general(
            left, right, (((0,), (0,)), ((), ())),
            precision=lax.Precision.HIGHEST, preferred_element_type=jnp.float32)

    b = b_ref[0]
    decay = column(decay_ref[0], jnp.ones_like(b))
    new = decay * state_ref[0] + column(inflow_ref[0], b)
    new_ref[0] = new
    c = jnp.broadcast_to(c_ref[0], (16, b.shape[1])).astype(jnp.bfloat16)
    y = lax.dot_general(
        c, new.astype(jnp.bfloat16), (((1,), (1,)), ((), ())), preferred_element_type=jnp.float32)
    y_ref[0] = y[0:1]


def state_step(decay, inflow, b_vals, c_vals, state):
    seqs, rows, size = state.shape
    row = lambda width: pl.BlockSpec((1, 1, width), lambda s: (s, 0, 0))
    block = pl.BlockSpec((1, rows, size), lambda s: (s, 0, 0))
    new, y = pl.pallas_call(
        state_kernel,
        grid=(seqs,),
        in_specs=[row(rows), row(rows), row(size), row(size), block],
        out_specs=[block, row(rows)],
        out_shape=[jax.ShapeDtypeStruct(state.shape, jnp.float32),
                   jax.ShapeDtypeStruct((seqs, 1, rows), jnp.float32)],
        name="state_step",
    )(decay[:, None], inflow[:, None], b_vals[:, None], c_vals[:, None], state)
    return new, y[:, 0]


def halves(column, lanes, first, split):
    high = column.astype(jnp.bfloat16).astype(jnp.float32)
    return jnp.where(lanes < split, high, column - high)


def tail_kernel(
    groups, heads, seqs,
    gated_ref, hid_ref, ngain_ref, fgain_ref, out_t_ref, lm_ref, refl_ref, token_ref, out_hbm,
    roll_out, result_ref,
    gall, hall, mix, pairs, pair_in, sums, sums_in, stat,
    gsend, grecv, hsend, hrecv, msend, mrecv, psend, precv, ssend, srecv, tsend, trecv,
    *gsems,
):
    chips = groups // 2
    group, head = lax.axis_index("group"), lax.axis_index("head")
    chip, core = group // 2, group % 2
    wide = mix.shape[2]
    depth = out_t_ref.shape[0]
    vocab = lm_ref.shape[0]
    rows = groups * seqs
    pending = []

    def send(src, dst, device, ssem, rsem):
        made = pltpu.make_async_remote_copy(
            src_ref=src, dst_ref=dst, send_sem=ssem, recv_sem=rsem, device_id=device, device_id_type=MESH)
        made.start()
        pending.append(made)
        return made

    work = Gather(chips, [out_hbm], [roll_out], *gsems)
    greet(groups, heads)
    first = []
    for j in range(1, groups):
        peer = (group + j) % groups
        first.append(send(gated_ref, gall.at[group], {"group": peer}, gsend.at[j], grecv.at[j]))
        first.append(send(hid_ref.at[peer], hall.at[group], {"group": peer}, hsend.at[j], hrecv.at[j]))
    work.start(0)
    gall[group] = gated_ref[...]
    hall[group] = hid_ref[group]
    for made in first:
        made.wait_recv()

    gated = gall[...].reshape(rows, gall.shape[2]).astype(jnp.float32)
    squares = jnp.sum(gated * gated, axis=-1, keepdims=True)
    scaled = (gated * ngain_ref[...]).astype(jnp.bfloat16)
    out_rows = out_t_ref[...]
    if wide > depth:
        out_rows = jnp.concatenate(
            [out_rows, jnp.zeros((wide - depth, out_rows.shape[1]), jnp.bfloat16)], axis=0)
    partial = lax.dot_general(
        scaled, out_rows, (((1,), (1,)), ((), ())), preferred_element_type=jnp.float32)
    lanes = lax.broadcasted_iota(jnp.int32, (rows, wide), 1)
    middle = (depth + wide) // 2
    mix[0] = jnp.where(lanes < depth, partial, halves(squares, lanes, depth, middle)).astype(jnp.bfloat16)
    mixes = [
        send(mix.at[0], mix.at[j], {"head": (head + j) % heads}, msend.at[j], mrecv.at[j])
        for j in range(1, heads)
    ]
    for made in mixes:
        made.wait_recv()
    work.relay_near(0)
    total = jnp.sum(mix[...].astype(jnp.float32), axis=0)
    square_total = total[:, depth:depth + 1] + total[:, middle:middle + 1]
    inner = gall.shape[2] * heads
    hidden = hall[...].reshape(rows, wide).astype(jnp.float32)
    stream = hidden + total * lax.rsqrt(square_total / inner + EPSILON)
    stream = jnp.where(lanes < depth, stream, 0.0)
    final_squares = jnp.sum(stream * stream, axis=-1, keepdims=True)
    final = (stream * fgain_ref[...]).astype(jnp.bfloat16)

    def by_core(values):
        parts = values.reshape(chips, 2, seqs, values.shape[1])
        return jnp.concatenate(
            [parts[:, 0].reshape(chips * seqs, -1), parts[:, 1].reshape(chips * seqs, -1)], axis=0)

    final = by_core(final.astype(jnp.float32)).astype(jnp.bfloat16)[:, :depth]
    final_squares = by_core(jnp.broadcast_to(final_squares, (rows, 128)))
    tail_lanes = lax.broadcasted_iota(jnp.int32, (rows, 128), 1)
    packed = halves(final_squares, tail_lanes, 0, 64).astype(jnp.bfloat16)
    half = chips * seqs
    for side in (0, 1):
        pairs[side, :, vocab:vocab + 128] = packed[side * half:(side + 1) * half]
    step_width = 640

    @pl.loop(0, vocab // step_width)
    def _(t):
        at = pl.ds(pl.multiple_of(t * step_width, step_width), step_width)
        block = lax.dot_general(
            final, lm_ref[at, :], (((1,), (1,)), ((), ())), preferred_element_type=jnp.float32)
        block = block.astype(jnp.bfloat16)
        pairs[0, :, at] = block[:half]
        pairs[1, :, at] = block[half:]

    pair = send(pairs.at[1 - core], pair_in, {"group": chip * 2 + 1 - core}, psend, precv)
    pair.wait_recv()
    joined = pairs[core].astype(jnp.float32) + pair_in[...].astype(jnp.float32)
    sums[:, :, :vocab] = joined[:, :vocab].astype(jnp.bfloat16).reshape(chips, seqs, vocab)
    rest = joined[:, vocab:]
    rest = rest[:, 0:1] + rest[:, 64:65]
    packed = halves(rest, lax.broadcasted_iota(jnp.int32, (half, 128), 1), 0, 64)
    sums[:, :, vocab:] = packed.astype(jnp.bfloat16).reshape(chips, seqs, 128)
    last = []
    for m in range(1, chips):
        peer = flip(chip, m)
        last.append(send(sums.at[peer], sums_in.at[m], {"group": peer * 2 + core}, ssend.at[m], srecv.at[m]))
    sums_in[0] = sums[chip]
    work.relay_far(0)
    for made in last:
        made.wait_recv()

    logits = jnp.sum(sums_in[...].astype(jnp.float32), axis=0)
    mean_square = (logits[:, vocab:vocab + 1] + logits[:, vocab + 64:vocab + 65]) / (depth * groups)
    logits = logits[:, :vocab] * lax.rsqrt(mean_square + EPSILON)
    reference = refl_ref[...].astype(jnp.float32)
    columns = lax.broadcasted_iota(jnp.int32, (seqs, vocab), 1) + head * vocab
    picked = jnp.sum(jnp.where(columns == token_ref[...], logits, 0.0), axis=-1, keepdims=True)
    top = jnp.max(logits, axis=-1, keepdims=True)
    ref_top = jnp.max(reference, axis=-1, keepdims=True)
    weights = jnp.exp(reference - ref_top)
    values = (
        top,
        jnp.sum(jnp.exp(logits - top), axis=-1, keepdims=True),
        ref_top,
        jnp.sum(weights, axis=-1, keepdims=True),
        jnp.sum(weights * (reference - logits), axis=-1, keepdims=True),
        picked,
    )
    slot = lax.broadcasted_iota(jnp.int32, (seqs, 128), 1)
    mine = jnp.zeros((seqs, 128), jnp.float32)
    for n, value in enumerate(values):
        mine = jnp.where(slot == n, value, mine)
    stat[0] = mine
    stats = [
        send(stat.at[0], stat.at[j], {"head": (head + j) % heads}, tsend.at[j], trecv.at[j])
        for j in range(1, heads)
    ]
    for made in stats:
        made.wait_recv()
    every = stat[...]
    pick = lambda n: every[:, :, n:n + 1]
    top = jnp.max(pick(0), axis=0)
    ref_top = jnp.max(pick(2), axis=0)
    factor = jnp.exp(pick(0) - top[None])
    ref_factor = jnp.exp(pick(2) - ref_top[None])
    roll_sum = jnp.sum(pick(1) * factor, axis=0)
    ref_sum = jnp.sum(pick(3) * ref_factor, axis=0)
    cross = jnp.sum(pick(4) * ref_factor, axis=0)
    picked = jnp.sum(pick(5), axis=0)
    lse_roll = top + jnp.log(roll_sum)
    lse_ref = ref_top + jnp.log(ref_sum)
    result_ref[...] = jnp.where(slot == 0, cross / ref_sum - lse_ref + lse_roll, picked - lse_roll)

    work.arrive(0)
    work.drain()
    for made in pending:
        made.wait_send()


def tail(groups, heads, gated, hid, ngain, fgain, out_t, lm_head, ref_logits, tokens):
    seqs, inner = gated.shape
    depth = out_t.shape[0]
    wide = hid.shape[2]
    vocab = lm_head.shape[0]
    chips = groups // 2
    vmem, any_spec = pl.BlockSpec(memory_space=pltpu.VMEM), pl.BlockSpec(memory_space=pl.ANY)
    dma = pltpu.SemaphoreType.DMA
    bf16 = jnp.bfloat16
    return pl.pallas_call(
        functools.partial(tail_kernel, groups, heads, seqs),
        out_shape=[jax.ShapeDtypeStruct((groups * depth, inner), bf16),
                   jax.ShapeDtypeStruct((seqs, 128), jnp.float32)],
        in_specs=[vmem] * 8 + [any_spec],
        out_specs=[any_spec, vmem],
        scratch_shapes=[
            pltpu.VMEM((groups, seqs, inner), bf16),
            pltpu.VMEM((groups, seqs, wide), bf16),
            pltpu.VMEM((heads, groups * seqs, wide), bf16),
            pltpu.VMEM((2, chips * seqs, vocab + 128), bf16),
            pltpu.VMEM((chips * seqs, vocab + 128), bf16),
            pltpu.VMEM((chips, seqs, vocab + 128), bf16),
            pltpu.VMEM((chips, seqs, vocab + 128), bf16),
            pltpu.VMEM((heads, seqs, 128), jnp.float32),
            dma((groups,)), dma((groups,)), dma((groups,)), dma((groups,)),
            dma((heads,)), dma((heads,)), dma, dma,
            dma((chips,)), dma((chips,)), dma((heads,)), dma((heads,)),
        ] + gather_sems(1, chips),
        compiler_params=pltpu.CompilerParams(
            collective_id=1, has_side_effects=True, vmem_limit_bytes=56 * 1024 * 1024),
        name="tail",
    )(gated, hid, ngain, fgain, out_t, lm_head, ref_logits, tokens, out_t)


def shards(
    groups, heads,
    hidden_in, ssm_state, conv_x_state, conv_bc_state, token_ids, ref_logits,
    in_z, in_x, in_bc, in_dt, out_t, lm_head,
    conv_wx, conv_bx, conv_wbc, conv_bbc, dt_bias, a_log, skip_gain, norm_in, norm_gain, final_gain,
):
    local_heads = a_log.shape[0]
    dt_wide = jnp.pad(in_dt, ((0, 0), (0, -in_dt.shape[1] % 128)))
    roll_bc, dt_all, roll_x, roll_z = gather(groups, [in_bc, dt_wide, in_x, in_z])
    roll_dt = dt_all[:, :local_heads]
    stream_in = hidden_in.astype(jnp.float32)
    normed = rms_norm(stream_in, norm_in).astype(jnp.bfloat16)
    gate_branch = jnp.dot(normed, roll_z, preferred_element_type=jnp.float32).astype(jnp.bfloat16)
    x_branch = jnp.dot(normed, roll_x, preferred_element_type=jnp.float32).astype(jnp.bfloat16)
    bc_branch = jnp.dot(normed, roll_bc, preferred_element_type=jnp.float32).astype(jnp.bfloat16)
    step_raw = jnp.dot(normed, dt_all, preferred_element_type=jnp.float32).astype(jnp.bfloat16)
    step_raw = step_raw[:, :local_heads]
    x_conv = causal_conv(conv_x_state, x_branch, conv_wx, conv_bx)
    bc_conv = causal_conv(conv_bc_state, bc_branch, conv_wbc, conv_bbc)
    state_size = bc_conv.shape[1] // 2
    b_vals = bc_conv[:, :state_size]
    c_vals = bc_conv[:, state_size:]
    step = jax.nn.softplus(step_raw.astype(jnp.float32) + dt_bias)
    decay = jnp.exp(-step * jnp.exp(a_log))
    seqs = x_conv.shape[0]
    inner = local_heads * P_SIZE
    spread = lambda v: jnp.repeat(v, P_SIZE, axis=-1)
    new_state, ssm_out = state_step(
        spread(decay), spread(step) * x_conv, b_vals, c_vals, ssm_state.reshape(seqs, inner, state_size))
    new_state = new_state.reshape(ssm_state.shape)
    ssm_out = ssm_out + spread(skip_gain)[None] * x_conv
    gated = (ssm_out * jax.nn.silu(gate_branch.astype(jnp.float32))).astype(jnp.bfloat16)
    depth = out_t.shape[0]
    extra = -depth % 128 or 128
    hid = hidden_in.reshape(seqs, groups, depth).transpose(1, 0, 2)
    hid = jnp.pad(hid, ((0, 0), (0, 0), (0, extra)))
    fgain = lax.dynamic_slice(final_gain, (lax.axis_index("group") * depth,), (depth,))
    fgain = jnp.pad(fgain, (0, extra))[None]
    roll_out, result = tail(
        groups, heads, gated, hid, norm_gain[None], fgain, out_t, lm_head, ref_logits, token_ids[:, None])
    return (new_state, result[:, 0], result[:, 1], roll_z, roll_x, roll_bc, roll_dt, roll_out)


def solution(mesh):
    return jax.shard_map(
        functools.partial(shards, mesh.shape["group"], mesh.shape["head"]),
        mesh=mesh,
        in_specs=(
            P("group", None),
            P("group", "head", None, None),
            P("group", None, "head"),
            P("group", None, None),
            P("group"),
            P("group", "head"),
            P("group", "head"),
            P("group", "head"),
            P("group", None),
            P("group", "head"),
            P("group", "head"),
            P("head", "group"),
            P(None, "head"),
            P("head"),
            P(),
            P(),
            P("head"),
            P("head"),
            P("head"),
            P(),
            P("head"),
            P(),
        ),
        out_specs=(
            P("group", "head", None, None),
            P("group"),
            P("group"),
            P(None, "head"),
            P(None, "head"),
            P(),
            P(None, "head"),
            P(None, "head"),
        ),
        check_vma=False,
    )
```

```python
import functools

import jax
import jax.numpy as jnp
from jax import lax
from jax.experimental import pallas as pl
from jax.experimental.pallas import tpu as pltpu
from jax.sharding import PartitionSpec as P

P_SIZE = 64
EPSILON = 1e-05
MESH = pl.DeviceIdType.MESH


def rms_norm(values, gain):
    return values * lax.rsqrt(jnp.mean(values * values, axis=-1, keepdims=True) + EPSILON) * gain


def causal_conv(history, newest, taps, offset):
    window = jnp.concatenate([history, newest[:, None, :]], axis=1).astype(jnp.float32)
    return jax.nn.silu(jnp.sum(window * taps[None, :, :], axis=1) + offset)


def flip(value, mask):
    bit = 1
    while bit <= mask:
        if mask & bit:
            value = value + bit * (1 - 2 * ((value // bit) % 2))
        bit *= 2
    return value


class Gather:
    def __init__(self, chips, ins, outs, local, send, recv, psend, precv):
        self.chips, self.ins, self.outs = chips, ins, outs
        self.local, self.send, self.recv, self.psend, self.precv = local, send, recv, psend, precv
        group = lax.axis_index("group")
        self.chip, self.core = group // 2, group % 2
        self.pending = []
        self.relay = chips == 4

    def rows(self, a, chip, core, part=None):
        count = self.ins[a].shape[0]
        start = (chip * 2 + core) * count
        if part is not None:
            count = count // 2
            start = start + part * count
        return pl.ds(pl.multiple_of(start, 16), count)

    def copy(self, src, dst, chip, core, ssem, rsem):
        made = pltpu.make_async_remote_copy(
            src_ref=src, dst_ref=dst, send_sem=ssem, recv_sem=rsem,
            device_id={"group": chip * 2 + core}, device_id_type=MESH,
        )
        made.start()
        self.pending.append(made)
        return made

    def start(self, a):
        src = self.ins[a]
        own = self.outs[a].at[self.rows(a, self.chip, self.core)]
        loc = pltpu.make_async_copy(src, own, self.local.at[a])
        loc.start()
        self.far = getattr(self, "far", {})
        peers = [1, 2] if self.relay else range(1, self.chips)
        for m in peers:
            self.far[a, m] = self.copy(
                src, own, flip(self.chip, m), self.core, self.send.at[a, m], self.recv.at[a, m])
        self.near = getattr(self, "near", {})
        self.near[a, 0] = self.copy(
            src, own, self.chip, 1 - self.core, self.psend.at[a, 0], self.precv.at[a, 0])
        self.locals = getattr(self, "locals", {})
        self.locals[a] = loc

    def hand_on(self, a, m, chip, part, slot):
        view = self.outs[a].at[self.rows(a, chip, self.core, part)]
        self.near[a, slot] = self.copy(
            view, view, self.chip, 1 - self.core, self.psend.at[a, slot], self.precv.at[a, slot])

    def relay_near(self, a):
        if self.relay:
            for m, part in ((1, 0), (2, 1)):
                self.far[a, m].wait_recv()
                source = flip(self.chip, m)
                view = self.outs[a].at[self.rows(a, source, self.core, part)]
                self.far[a, 3 + part] = self.copy(
                    view, view, flip(self.chip, 3 - m), self.core,
                    self.send.at[a, 3 + part], self.recv.at[a, 3 + part])
                self.hand_on(a, m, source, None, m)
        else:
            for m in range(1, self.chips):
                self.far[a, m].wait_recv()
                self.hand_on(a, m, flip(self.chip, m), None, m)

    def relay_far(self, a):
        if self.relay:
            for part in (0, 1):
                self.far[a, 3 + part].wait_recv()
                self.hand_on(a, 3, flip(self.chip, 3), part, 3 + part)

    def arrive(self, a):
        for (b, _), made in self.near.items():
            if b == a:
                made.wait_recv()
        self.locals[a].wait()

    def drain(self):
        for made in self.pending:
            made.wait_send()


def gather_sems(count, chips):
    slots = max(chips, 5)
    dma = pltpu.SemaphoreType.DMA
    return [dma((count,)), dma((count, slots)), dma((count, slots)), dma((count, slots)), dma((count, slots))]


def greet(groups, heads):
    barrier = pltpu.get_barrier_semaphore()
    group, head = lax.axis_index("group"), lax.axis_index("head")
    for j in range(1, groups):
        pl.semaphore_signal(barrier, inc=1, device_id={"group": (group + j) % groups}, device_id_type=MESH)
    for j in range(1, heads):
        pl.semaphore_signal(barrier, inc=1, device_id={"head": (head + j) % heads}, device_id_type=MESH)
    pl.semaphore_wait(barrier, groups - 1 + heads - 1)


def gather_kernel(groups, count, *refs):
    ins, outs, sems = refs[:count], refs[count:2 * count], refs[2 * count:]
    work = Gather(groups // 2, ins, outs, *sems)
    greet(groups, 1)
    for a in range(count):
        work.start(a)
    for a in range(count):
        work.relay_near(a)
        if a:
            work.relay_far(a - 1)
    work.relay_far(count - 1)
    for a in range(count):
        work.arrive(a)
    work.drain()


def gather(groups, arrays):
    count = len(arrays)
    any_spec = pl.BlockSpec(memory_space=pl.ANY)
    return pl.pallas_call(
        functools.partial(gather_kernel, groups, count),
        out_shape=[jax.ShapeDtypeStruct((groups * v.shape[0], v.shape[1]), v.dtype) for v in arrays],
        in_specs=[any_spec] * count,
        out_specs=[any_spec] * count,
        scratch_shapes=gather_sems(count, groups // 2),
        compiler_params=pltpu.CompilerParams(collective_id=0, has_side_effects=True),
        name="gather_in",
    )(*arrays)


def project_kernel(steps, normed_ref, *refs):
    count = len(refs) // 4
    weights, sums, copies, totals = (refs[n * count:(n + 1) * count] for n in range(4))
    step = pl.program_id(0)

    @pl.when(step == 0)
    def _():
        for total in totals:
            total[...] = jnp.zeros_like(total)

    for weight, copied, total in zip(weights, copies, totals):
        block = weight[...]
        copied[...] = block
        total[...] += jnp.dot(normed_ref[...], block, preferred_element_type=jnp.float32)

    @pl.when(step == steps - 1)
    def _():
        for out, total in zip(sums, totals):
            out[...] = total[...].astype(out.dtype)


def project(normed, weights):
    seqs, depth = normed.shape
    steps = 5
    rows = depth // steps
    whole = lambda w: pl.BlockSpec((seqs, w.shape[1]), lambda k: (0, 0))
    block = lambda w: pl.BlockSpec((rows, w.shape[1]), lambda k: (k, 0))
    made = pl.pallas_call(
        functools.partial(project_kernel, steps),
        grid=(steps,),
        in_specs=[pl.BlockSpec((seqs, rows), lambda k: (0, k))] + [block(w) for w in weights],
        out_specs=[whole(w) for w in weights] + [block(w) for w in weights],
        out_shape=[jax.ShapeDtypeStruct((seqs, w.shape[1]), jnp.bfloat16) for w in weights]
        + [jax.ShapeDtypeStruct(w.shape, w.dtype) for w in weights],
        scratch_shapes=[pltpu.VMEM((seqs, w.shape[1]), jnp.float32) for w in weights],
        name="project",
    )(normed, *weights)
    return made[:len(weights)], made[len(weights):]


def state_kernel(each, decay_ref, inflow_ref, b_ref, c_ref, state_ref, new_ref, y_ref):
    heads, width, size = state_ref.shape[1:]

    def pair(row):
        high = row.astype(jnp.bfloat16).astype(jnp.float32)
        return high, row - high

    for n in range(each):
        seq = pl.program_id(0) * each + n
        high, low = pair(inflow_ref[n])
        b_high, b_low = pair(b_ref[n])
        place = lax.broadcasted_iota(jnp.int32, (16, heads * width), 0)
        left = jnp.where(place < 2, high, jnp.where(place < 4, low, 0.0)).astype(jnp.bfloat16)
        place = lax.broadcasted_iota(jnp.int32, (16, size), 0)
        right = jnp.where(place % 2 == 0, b_high, b_low).astype(jnp.bfloat16)
        inflow = lax.dot_general(
            left, right, (((0,), (0,)), ((), ())), preferred_element_type=jnp.float32)
        for h in range(heads):
            new_ref[n, h] = decay_ref[seq, h] * state_ref[n, h] + inflow[h * width:(h + 1) * width]
        new = new_ref[n].reshape(heads * width, size).astype(jnp.bfloat16)
        c = jnp.broadcast_to(c_ref[n], (16, size)).astype(jnp.bfloat16)
        y = lax.dot_general(c, new, (((1,), (1,)), ((), ())), preferred_element_type=jnp.float32)
        y_ref[n] = y[0:1]


def state_step(decay, inflow, b_vals, c_vals, state):
    seqs, heads, width, size = state.shape
    each = 2
    row = lambda wide: pl.BlockSpec((each, 1, wide), lambda s: (s, 0, 0))
    block = pl.BlockSpec((each, heads, width, size), lambda s: (s, 0, 0, 0))
    new, y = pl.pallas_call(
        functools.partial(state_kernel, each),
        grid=(seqs // each,),
        in_specs=[pl.BlockSpec(memory_space=pltpu.SMEM), row(heads * width), row(size), row(size), block],
        out_specs=[block, row(heads * width)],
        out_shape=[jax.ShapeDtypeStruct(state.shape, jnp.float32),
                   jax.ShapeDtypeStruct((seqs, 1, heads * width), jnp.float32)],
        name="state_step",
    )(decay, inflow[:, None], b_vals[:, None], c_vals[:, None], state)
    return new, y[:, 0]


def halves(column, lanes, first, split):
    high = column.astype(jnp.bfloat16).astype(jnp.float32)
    return jnp.where(lanes < split, high, column - high)


def tail_kernel(
    groups, heads, seqs,
    gated_ref, hid_ref, ngain_ref, fgain_ref, out_t_ref, lm_ref, refl_ref, token_ref, out_hbm,
    roll_out, result_ref,
    gall, hall, mix, pairs, pair_in, sums, sums_in, square, square_in, squares_out, squares_in, stat,
    gsend, grecv, hsend, hrecv, msend, mrecv, psend, precv, ssend, srecv, tsend, trecv,
    *gsems,
):
    chips = groups // 2
    group, head = lax.axis_index("group"), lax.axis_index("head")
    chip, core = group // 2, group % 2
    wide = mix.shape[2]
    depth = out_t_ref.shape[0]
    vocab = lm_ref.shape[1]
    parts = pairs.shape[0]
    width = vocab // parts
    rows = groups * seqs
    pending = []

    def send(src, dst, device, ssem, rsem):
        made = pltpu.make_async_remote_copy(
            src_ref=src, dst_ref=dst, send_sem=ssem, recv_sem=rsem, device_id=device, device_id_type=MESH)
        made.start()
        pending.append(made)
        return made

    work = Gather(chips, [out_hbm], [roll_out], *gsems)
    greet(groups, heads)
    first = []
    for j in range(1, groups):
        peer = (group + j) % groups
        first.append(send(gated_ref, gall.at[group], {"group": peer}, gsend.at[j], grecv.at[j]))
        first.append(send(hid_ref.at[peer], hall.at[group], {"group": peer}, hsend.at[j], hrecv.at[j]))
    work.start(0)
    gall[group] = gated_ref[...]
    hall[group] = hid_ref[group]
    for made in first:
        made.wait_recv()

    gated = gall[...].reshape(rows, gall.shape[2]).astype(jnp.float32)
    squares = jnp.sum(gated * gated, axis=-1, keepdims=True)
    scaled = (gated * ngain_ref[...]).astype(jnp.bfloat16)
    out_rows = out_t_ref[...]
    if wide > depth:
        out_rows = jnp.concatenate(
            [out_rows, jnp.zeros((wide - depth, out_rows.shape[1]), jnp.bfloat16)], axis=0)
    partial = lax.dot_general(
        scaled, out_rows, (((1,), (1,)), ((), ())), preferred_element_type=jnp.float32)
    lanes = lax.broadcasted_iota(jnp.int32, (rows, wide), 1)
    middle = (depth + wide) // 2
    mix[0] = jnp.where(lanes < depth, partial, halves(squares, lanes, depth, middle)).astype(jnp.bfloat16)
    mixes = [
        send(mix.at[0], mix.at[j], {"head": (head + j) % heads}, msend.at[j], mrecv.at[j])
        for j in range(1, heads)
    ]
    for made in mixes:
        made.wait_recv()
    work.relay_near(0)
    total = jnp.sum(mix[...].astype(jnp.float32), axis=0)
    square_total = total[:, depth:depth + 1] + total[:, middle:middle + 1]
    inner = gall.shape[2] * heads
    hidden = hall[...].reshape(rows, wide).astype(jnp.float32)
    stream = hidden + total * lax.rsqrt(square_total / inner + EPSILON)
    stream = jnp.where(lanes < depth, stream, 0.0)
    final_squares = jnp.sum(stream * stream, axis=-1, keepdims=True)
    final = (stream * fgain_ref[...]).astype(jnp.bfloat16)

    def by_core(values):
        parts = values.reshape(chips, 2, seqs, values.shape[1])
        return jnp.concatenate(
            [parts[:, 0].reshape(chips * seqs, -1), parts[:, 1].reshape(chips * seqs, -1)], axis=0)

    final = by_core(final.astype(jnp.float32)).astype(jnp.bfloat16)[:, :depth]
    final_squares = by_core(jnp.broadcast_to(final_squares, (rows, 128)))
    tail_lanes = lax.broadcasted_iota(jnp.int32, (rows, 128), 1)
    packed = halves(final_squares, tail_lanes, 0, 64).astype(jnp.bfloat16)
    half = chips * seqs
    other = {"group": chip * 2 + 1 - core}
    square[0], square[1] = packed[:half], packed[half:]
    pair_sends = [send(square.at[1 - core], square_in, other, psend.at[parts], precv.at[parts])]
    last = []

    def out(source, target, t):
        for m in range(1, chips):
            peer = flip(chip, m)
            last.append(send(
                source.at[peer], target.at[m], {"group": peer * 2 + core}, ssend.at[t, m], srecv.at[t, m]))
        target[0] = source[chip]

    def join(t):
        pair_sends[t + 1].wait_recv()
        joined = pairs[t, core].astype(jnp.float32) + pair_in[t].astype(jnp.float32)
        sums[t] = joined.astype(jnp.bfloat16).reshape(chips, seqs, width)
        out(sums.at[t], sums_in.at[t], t)

    for t in range(parts):
        block = lax.dot_general(
            final, lm_ref[:, t * width:(t + 1) * width], (((1,), (0,)), ((), ())),
            preferred_element_type=jnp.float32).astype(jnp.bfloat16)
        pairs[t, 0], pairs[t, 1] = block[:half], block[half:]
        pair_sends.append(send(pairs.at[t, 1 - core], pair_in.at[t], other, psend.at[t], precv.at[t]))
        if t == 0:
            pair_sends[0].wait_recv()
            rest = square[core].astype(jnp.float32) + square_in[...].astype(jnp.float32)
            rest = rest[:, 0:1] + rest[:, 64:65]
            split = halves(rest, lax.broadcasted_iota(jnp.int32, (half, 128), 1), 0, 64)
            squares_out[...] = split.astype(jnp.bfloat16).reshape(chips, seqs, 128)
            out(squares_out, squares_in, parts)
        else:
            join(t - 1)
    join(parts - 1)
    work.relay_far(0)
    for made in last:
        made.wait_recv()

    square_sum = jnp.sum(squares_in[...].astype(jnp.float32), axis=0)
    mean_square = (square_sum[:, 0:1] + square_sum[:, 64:65]) / (depth * groups)
    logits = jnp.concatenate(
        [jnp.sum(sums_in[t].astype(jnp.float32), axis=0) for t in range(parts)], axis=1)
    logits = logits * lax.rsqrt(mean_square + EPSILON)
    reference = refl_ref[...].astype(jnp.float32)
    columns = lax.broadcasted_iota(jnp.int32, (seqs, vocab), 1) + head * vocab
    picked = jnp.sum(jnp.where(columns == token_ref[...], logits, 0.0), axis=-1, keepdims=True)
    top = jnp.max(logits, axis=-1, keepdims=True)
    ref_top = jnp.max(reference, axis=-1, keepdims=True)
    weights = jnp.exp(reference - ref_top)
    values = (
        top,
        jnp.sum(jnp.exp(logits - top), axis=-1, keepdims=True),
        ref_top,
        jnp.sum(weights, axis=-1, keepdims=True),
        jnp.sum(weights * (reference - logits), axis=-1, keepdims=True),
        picked,
    )
    slot = lax.broadcasted_iota(jnp.int32, (seqs, 128), 1)
    mine = jnp.zeros((seqs, 128), jnp.float32)
    for n, value in enumerate(values):
        mine = jnp.where(slot == n, value, mine)
    stat[0] = mine
    stats = [
        send(stat.at[0], stat.at[j], {"head": (head + j) % heads}, tsend.at[j], trecv.at[j])
        for j in range(1, heads)
    ]
    for made in stats:
        made.wait_recv()
    every = stat[...]
    pick = lambda n: every[:, :, n:n + 1]
    top = jnp.max(pick(0), axis=0)
    ref_top = jnp.max(pick(2), axis=0)
    factor = jnp.exp(pick(0) - top[None])
    ref_factor = jnp.exp(pick(2) - ref_top[None])
    roll_sum = jnp.sum(pick(1) * factor, axis=0)
    ref_sum = jnp.sum(pick(3) * ref_factor, axis=0)
    cross = jnp.sum(pick(4) * ref_factor, axis=0)
    picked = jnp.sum(pick(5), axis=0)
    lse_roll = top + jnp.log(roll_sum)
    lse_ref = ref_top + jnp.log(ref_sum)
    result_ref[...] = jnp.where(slot == 0, cross / ref_sum - lse_ref + lse_roll, picked - lse_roll)

    work.arrive(0)
    work.drain()
    for made in pending:
        made.wait_send()


def tail(groups, heads, gated, hid, ngain, fgain, out_t, lm_head, ref_logits, tokens):
    seqs, inner = gated.shape
    depth = out_t.shape[0]
    wide = hid.shape[2]
    vocab = lm_head.shape[1]
    parts = 5
    width = vocab // parts
    chips = groups // 2
    vmem, any_spec = pl.BlockSpec(memory_space=pltpu.VMEM), pl.BlockSpec(memory_space=pl.ANY)
    dma = pltpu.SemaphoreType.DMA
    bf16 = jnp.bfloat16
    return pl.pallas_call(
        functools.partial(tail_kernel, groups, heads, seqs),
        out_shape=[jax.ShapeDtypeStruct((groups * depth, inner), bf16),
                   jax.ShapeDtypeStruct((seqs, 128), jnp.float32)],
        in_specs=[vmem] * 8 + [any_spec],
        out_specs=[any_spec, vmem],
        scratch_shapes=[
            pltpu.VMEM((groups, seqs, inner), bf16),
            pltpu.VMEM((groups, seqs, wide), bf16),
            pltpu.VMEM((heads, groups * seqs, wide), bf16),
            pltpu.VMEM((parts, 2, chips * seqs, width), bf16),
            pltpu.VMEM((parts, chips * seqs, width), bf16),
            pltpu.VMEM((parts, chips, seqs, width), bf16),
            pltpu.VMEM((parts, chips, seqs, width), bf16),
            pltpu.VMEM((2, chips * seqs, 128), bf16),
            pltpu.VMEM((chips * seqs, 128), bf16),
            pltpu.VMEM((chips, seqs, 128), bf16),
            pltpu.VMEM((chips, seqs, 128), bf16),
            pltpu.VMEM((heads, seqs, 128), jnp.float32),
            dma((groups,)), dma((groups,)), dma((groups,)), dma((groups,)),
            dma((heads,)), dma((heads,)), dma((parts + 1,)), dma((parts + 1,)),
            dma((parts + 1, chips)), dma((parts + 1, chips)), dma((heads,)), dma((heads,)),
        ] + gather_sems(1, chips),
        compiler_params=pltpu.CompilerParams(
            collective_id=1, has_side_effects=True, vmem_limit_bytes=56 * 1024 * 1024),
        name="tail",
    )(gated, hid, ngain, fgain, out_t, lm_head, ref_logits, tokens, out_t)


def shards(
    groups, heads,
    hidden_in, ssm_state, conv_x_state, conv_bc_state, token_ids, ref_logits,
    in_z, in_x, in_bc, in_dt, out_t, lm_head,
    conv_wx, conv_bx, conv_wbc, conv_bbc, dt_bias, a_log, skip_gain, norm_in, norm_gain, final_gain,
):
    local_heads = a_log.shape[0]
    dt_wide = jnp.pad(in_dt, ((0, 0), (0, -in_dt.shape[1] % 128)))
    roll_bc, dt_all, roll_x, roll_z = gather(groups, [in_bc, dt_wide, in_x, in_z])
    stream_in = hidden_in.astype(jnp.float32)
    normed = rms_norm(stream_in, norm_in).astype(jnp.bfloat16)
    (gate_branch, x_branch, bc_branch, step_raw), (roll_z, roll_x, roll_bc, dt_all) = project(
        normed, (roll_z, roll_x, roll_bc, dt_all))
    roll_dt = dt_all[:, :local_heads]
    step_raw = step_raw[:, :local_heads]
    x_conv = causal_conv(conv_x_state, x_branch, conv_wx, conv_bx)
    bc_conv = causal_conv(conv_bc_state, bc_branch, conv_wbc, conv_bbc)
    state_size = bc_conv.shape[1] // 2
    b_vals = bc_conv[:, :state_size]
    c_vals = bc_conv[:, state_size:]
    step = jax.nn.softplus(step_raw.astype(jnp.float32) + dt_bias)
    decay = jnp.exp(-step * jnp.exp(a_log))
    seqs = x_conv.shape[0]
    spread = lambda v: jnp.repeat(v, P_SIZE, axis=-1)
    new_state, ssm_out = state_step(
        decay, spread(step) * x_conv, b_vals, c_vals, ssm_state)
    ssm_out = ssm_out + spread(skip_gain)[None] * x_conv
    gated = (ssm_out * jax.nn.silu(gate_branch.astype(jnp.float32))).astype(jnp.bfloat16)
    depth = out_t.shape[0]
    extra = -depth % 128 or 128
    hid = hidden_in.reshape(seqs, groups, depth).transpose(1, 0, 2)
    hid = jnp.pad(hid, ((0, 0), (0, 0), (0, extra)))
    fgain = lax.dynamic_slice(final_gain, (lax.axis_index("group") * depth,), (depth,))
    fgain = jnp.pad(fgain, (0, extra))[None]
    roll_out, result = tail(
        groups, heads, gated, hid, norm_gain[None], fgain, out_t, lm_head.T, ref_logits, token_ids[:, None])
    return (new_state, result[:, 0], result[:, 1], roll_z, roll_x, roll_bc, roll_dt, roll_out)


def solution(mesh):
    return jax.shard_map(
        functools.partial(shards, mesh.shape["group"], mesh.shape["head"]),
        mesh=mesh,
        in_specs=(
            P("group", None),
            P("group", "head", None, None),
            P("group", None, "head"),
            P("group", None, None),
            P("group"),
            P("group", "head"),
            P("group", "head"),
            P("group", "head"),
            P("group", None),
            P("group", "head"),
            P("group", "head"),
            P("head", "group"),
            P(None, "head"),
            P("head"),
            P(),
            P(),
            P("head"),
            P("head"),
            P("head"),
            P(),
            P("head"),
            P(),
        ),
        out_specs=(
            P("group", "head", None, None),
            P("group"),
            P("group"),
            P(None, "head"),
            P(None, "head"),
            P(),
            P(None, "head"),
            P(None, "head"),
        ),
        check_vma=False,
    )
```
